512 devices in a mesh: dp: 64 (over z, y), member: 8 (over x, core).
Axes of the slice: x: 4, y: 8, z: 8, core: 2. Of those that a mesh axis runs over, the one named last changes fastest.
Arguments:
- inputs: bfloat16 [98304, 393], P(('dp', 'member')), may hold values from -256 to 256
- targets: bfloat16 [98304, 377], P(('dp', 'member')), may hold values from -6 to 6
- bootstrap: int32 [8, 98304], P('member', 'dp'), may hold values from 0 to 1535
- lower_weight: bfloat16 [8, 393, 1024], P('member'), may hold values from -0.3125 to 0.3125
- lower_shift: float32 [8, 1024], P('member'), may hold values from -3 to 3
- upper_weight: bfloat16 [8, 1024, 377], P('member'), may hold values from -0.1875 to 0.1875
- upper_shift: float32 [8, 377], P('member'), may hold values from -3 to 3
- log_var: float32 [8, 377], P('member'), may hold values from -1 to 1
Outputs:
- lower_grad: float32 [8, 1024, 393], P('member', 'dp')
- bias_grad: float32 [8, 1024], P('member', 'dp')
- upper_grad: float32 [8, 1024, 377], P('member', 'dp')
- offset_grad: float32 [8, 377], P('member')
- noise_grad: float32 [8, 377], P('member')
- member_loss: float32 [8], P('member')
The draws below stay inside these ranges and needn't reach their ends.
Inputs may be any that keep to these rules, and one draw needn't show every extreme that they name: bootstrap[m, r] is an offset within the aligned block of 1536 rows that holds row r.
All inputs are finite; a program needn't handle non-finite values.
Results may differ from the reference program's by a relative error of at most 0.00076.
Values may be sent and summed in bfloat16 or wider, within the bound.
No kernel may reach another device: no remote copies, remote signals or barrier semaphores. Data moves between devices by JAX's collectives and lax.ppermute only.
A program may use at most 64 MiB of HBM per device.

```python
import math
import jax
import jax.numpy as jnp
from jax import lax

IN = 393
OUT = 377
H = 1024
ROWS_DEV = 1536
MEMBERS = 8
ROWS = 98304
N_DP = 64


def draw_inputs(key, part):
    keys = jax.random.split(key, 4)
    position = jnp.arange(ROWS, dtype=jnp.float32) / ROWS
    rising = (1.0 + 2.0 * position)[:, None]
    column_scale = jnp.exp(jax.random.uniform(keys[1], (1, IN), jnp.float32, math.log(0.3), math.log(3.0)))
    offset = jax.random.uniform(keys[2], (1, IN), jnp.float32, -1.0, 1.0)
    row_scale = jnp.exp(jax.random.uniform(keys[0], (ROWS, 1), jnp.float32, math.log(0.5), math.log(5.0)))
    noise = jax.random.truncated_normal(keys[3], -4.0, 4.0, (ROWS, IN), jnp.float32)
    return ((noise + offset) * row_scale * rising * column_scale).astype(jnp.bfloat16)


def set_ends(values, own_key, smallest, high):
    shape = values.shape
    index_at = [jax.random.randint(jax.random.fold_in(own_key, axis), (), 0, shape[axis]) for axis in range(len(shape))]
    values = values.at[tuple(index_at)].set(smallest)
    longest = shape.index(max(shape))
    index_at[longest] = (index_at[longest] + 1) % shape[longest]
    return values.at[tuple(index_at)].set(high)


def block_levels(key, extent, cuts, low, high):
    def one(dim, parts):
        heights = jax.random.uniform(jax.random.fold_in(jax.random.fold_in(key, 6), dim), (parts,), jnp.float32, low / len(cuts), high / len(cuts))
        return jnp.repeat(jnp.exp(heights), extent[dim] // parts).reshape((-1,) + (1,) * (len(extent) - dim - 1))

    gain = one(*cuts[0])
    for cut in cuts[1:]:
        gain = gain * one(*cut)
    return gain


def scatter_about(rng, dims, spread, reach, cuts=(), kind=jnp.bfloat16):
    result = jax.random.normal(rng, dims, jnp.float32) * spread
    if len(cuts) > 0:
        result = block_levels(rng, dims, cuts, -0.22, 0.18) * result
    return jnp.clip(result, min=-reach, max=reach).astype(kind)


def setup_inputs(seed: int = 0) -> dict:
    splits = jax.random.split(jax.random.key(seed), 9)
    inputs = draw_inputs(jax.random.fold_in(splits[8], 71), 0)
    targets = scatter_about(splits[1], (ROWS, OUT), 1.0, 6.0, ((0, 512),))
    bootstrap = set_ends(jax.random.randint(splits[2], (MEMBERS, ROWS), 0, ROWS_DEV), jax.random.fold_in(splits[2], 1), 0, ROWS_DEV - 1).astype(jnp.int32)
    lower_weight = scatter_about(splits[3], (MEMBERS, IN, H), IN ** -0.5, 0.3125, ((0, 8),))
    lower_shift = scatter_about(splits[4], (MEMBERS, H), 0.5, 3.0, ((0, 8),), jnp.float32)
    upper_weight = scatter_about(splits[5], (MEMBERS, H, OUT), H ** -0.5, 0.1875, ((0, 8),))
    upper_shift = scatter_about(splits[6], (MEMBERS, OUT), 0.5, 3.0, ((0, 8),), jnp.float32)
    log_var = jnp.clip(jax.random.uniform(splits[7], (MEMBERS, OUT), jnp.float32, -1.0, 1.0) * block_levels(splits[7], (MEMBERS, OUT), ((0, 8),), -0.4, 0.0), -1.0, 1.0)
    return {"inputs": inputs, "targets": targets, "bootstrap": bootstrap, "lower_weight": lower_weight, "lower_shift": lower_shift, "upper_weight": upper_weight, "upper_shift": upper_shift, "log_var": log_var}


def member_terms(picked, goal_rows, lower_weight, lower_shift, upper_weight, upper_shift, log_var, row_count):
    pre_act = jnp.dot(picked, lower_weight, preferred_element_type=jnp.float32) + lower_shift
    hidden = jax.nn.silu(pre_act).astype(jnp.bfloat16)
    pred_mean = jnp.dot(hidden, upper_weight, preferred_element_type=jnp.float32) + upper_shift
    residual = pred_mean - goal_rows.astype(jnp.float32)
    scaled_err = residual * jnp.exp(-log_var)
    member_loss = 0.5 * jnp.sum(residual * scaled_err + log_var) / row_count
    grad_mean = scaled_err / row_count
    offset_grad = lax.optimization_barrier(jnp.sum(grad_mean, axis=0))
    noise_grad = 0.5 * lax.optimization_barrier(jnp.sum(1.0 - residual * scaled_err, axis=0)) / row_count
    grad_half = grad_mean.astype(jnp.bfloat16)
    upper_grad = lax.dot_general(hidden, grad_half, (((0,), (0,)), ((), ())), preferred_element_type=jnp.float32)
    grad_hidden = lax.dot_general(grad_half, upper_weight, (((1,), (1,)), ((), ())), preferred_element_type=jnp.float32)
    gate_sig = jax.nn.sigmoid(pre_act)
    grad_pre = grad_hidden * gate_sig * (1.0 + pre_act * (1.0 - gate_sig))
    bias_grad = lax.optimization_barrier(jnp.sum(grad_pre, axis=0))
    pre_half = grad_pre.astype(jnp.bfloat16)
    lower_grad = lax.dot_general(pre_half, picked, (((0,), (0,)), ((), ())), preferred_element_type=jnp.float32)
    return (lower_grad, bias_grad, upper_grad, offset_grad, noise_grad, member_loss)

def stack_all(*pieces):
    return jnp.stack(pieces)

def reference(inputs, targets, bootstrap, lower_weight, lower_shift, upper_weight, upper_shift, log_var):
    values = inputs.astype(jnp.float32)
    feature_mean = lax.optimization_barrier(jnp.sum(values, axis=0)) / ROWS
    centered = values - feature_mean
    feature_var = lax.optimization_barrier(jnp.sum(centered * centered, axis=0)) / ROWS
    feature_scale = 1.0 / jnp.sqrt(feature_var + 1e-06)
    scaled = (centered * feature_scale).astype(jnp.bfloat16)
    row_blocks = scaled.reshape(N_DP, ROWS_DEV, IN)
    goal_blocks = targets.reshape(N_DP, ROWS_DEV, OUT)
    pick_blocks = bootstrap.reshape(MEMBERS, N_DP, ROWS_DEV)
    results = []
    for member in range(MEMBERS):

        def visit_block(running, block_items, member=member):
            row_block, goal_block, pick_row = block_items
            block_terms = member_terms(row_block[pick_row], goal_block[pick_row], lower_weight[member], lower_shift[member], upper_weight[member], upper_shift[member], log_var[member], ROWS_DEV)
            return (jax.tree.map(jnp.add, running, block_terms), None)
        zero_sums = (jnp.zeros((H, IN), jnp.float32), jnp.zeros((H,), jnp.float32), jnp.zeros((H, OUT), jnp.float32), jnp.zeros((OUT,), jnp.float32), jnp.zeros((OUT,), jnp.float32), jnp.zeros((), jnp.float32))
        totals, unused = lax.scan(visit_block, zero_sums, (row_blocks, goal_blocks, pick_blocks[member]))
        results.append(totals)
    lower_grad, bias_grad, upper_grad, offset_grad, noise_grad, member_loss = jax.tree.map(stack_all, *results)
    return (lower_grad, bias_grad, upper_grad, offset_grad, noise_grad, member_loss)
```

```python
import jax
import jax.numpy as jnp
from jax import lax
from jax.experimental import pallas as pl
from jax.experimental.pallas import tpu as pltpu
from jax.sharding import Mesh
from jax.sharding import PartitionSpec as P


IN, OUT, H = 393, 377, 1024
IN_PAD, OUT_PAD = 512, 384
ROWS = 1536
PIECE = 192
TOTAL = 98304
CHUNK = 256
TILE = 112
DP = ("dp_0", "dp_1")
MEMBER = ("member_0", "member_1")
ALL = ("dp_0", "dp_1", "member_0", "member_1")
BF16, F32 = jnp.bfloat16, jnp.float32


def groups_by(key):
    found = {}
    for z in range(8):
        for y in range(8):
            for x in range(4):
                for c in range(2):
                    found.setdefault(key(z, y, x, c), []).append(((z * 8 + y) * 4 + x) * 2 + c)
    return list(found.values())


FIRST = groups_by(lambda z, y, x, c: (c, x, y) if c == 0 else (c, x, z))
SECOND = groups_by(lambda z, y, x, c: (c, x, z) if c == 0 else (c, x, y))


def vmem(n):
    return [pl.BlockSpec(memory_space=pltpu.VMEM)] * n


def call(body, outs, n_in, scratch=(), flops=0, moved=0):
    return pl.pallas_call(
        body,
        out_shape=outs,
        in_specs=vmem(n_in),
        out_specs=jax.tree.map(lambda _: pl.BlockSpec(memory_space=pltpu.VMEM), outs),
        scratch_shapes=list(scratch),
        compiler_params=pltpu.CompilerParams(vmem_limit_bytes=48 * 1024 * 1024),
        cost_estimate=pl.CostEstimate(flops=flops, bytes_accessed=moved, transcendentals=0),
    )


def shape(*dims, dtype=F32):
    return jax.ShapeDtypeStruct(dims, dtype)


def prepare_body(inputs, targets, both, stats):
    x = inputs[...]
    both[:, 384:512] = jnp.zeros((PIECE, 128), BF16)
    both[:, 768:896] = jnp.zeros((PIECE, 128), BF16)
    both[:, 0:IN] = x
    both[:, 512 : 512 + OUT] = targets[...]
    stats[...] = jnp.zeros(stats.shape, F32)
    for t in range(4):
        width = min(128, IN - 128 * t)
        v = inputs[:, 128 * t : 128 * t + width].astype(F32)
        mean = jnp.sum(v, axis=0, keepdims=True) * (1.0 / PIECE)
        centred = v - mean
        square = jnp.sum(centred * centred, axis=0, keepdims=True)
        for i in range(stats.shape[0]):
            stats[i, t : t + 1, 0:width] = mean
            stats[i, 4 + t : 5 + t, 0:width] = square


def merged(stats, rows_each):
    means, squares = stats[:, 0:4, :], stats[:, 4:8, :]
    mean = jnp.sum(means, axis=0) * (1.0 / stats.shape[0])
    away = means - mean[None]
    return mean, jnp.sum(squares, axis=0) + rows_each * jnp.sum(away * away, axis=0)


def merge_body(stats, out):
    mean, square = merged(stats[...], float(PIECE))
    for i in range(out.shape[0]):
        out[i, 0:4, :] = mean
        out[i, 4:8, :] = square


def counts_body(bootstrap, col, row):
    x, c = lax.axis_index("member_0"), lax.axis_index("member_1")
    shift = []
    for p in range(8):
        core = c if p < 4 else 1 - c
        member = lax.rem(x + 4 - p % 4, 4) * 2 + core
        shift.append((member - p) * PIECE)
    picks = bootstrap[...]
    for k in range(ROWS // 128):
        first, last = 128 * k // PIECE, (128 * k + 127) // PIECE
        place = lax.broadcasted_iota(jnp.int32, (128, 1), 0) + 128 * k
        row_id = place + jnp.where(place < PIECE * (first + 1), shift[first], shift[last])
        hits = (picks == row_id).astype(F32)
        total = jnp.sum(hits, axis=1, keepdims=True)
        wide = jnp.broadcast_to(total, (128, 128))
        row[:, 128 * k : 128 * k + 128] = wide.T[0:8, :]
    del col


def column(ref, lane):
    return ref[:, lane : lane + 1]


def step_body(
    mine, other, stats, counts, w1t, w2, w2t, cols_h, cols_o, send, xs, hidden, slope, grads, weighted, pre, goal_t
):
    mean, square = merged(stats[...], float(PIECE * 16))
    scale = 1.0 / jnp.sqrt(square * (1.0 / TOTAL) + 1e-06)
    for t in range(4):
        m, s = mean[t : t + 1, :], scale[t : t + 1, :]
        lanes = slice(128 * t, 128 * t + 128)
        for half, src in enumerate((mine, other)):
            v = (src[:, lanes].astype(F32) - m) * s
            xs[768 * half : 768 * half + 768, lanes] = v.astype(BF16)
    bias_h = column(cols_h, 0)
    bias_o, log_var = column(cols_o, 0), column(cols_o, 1)
    shrink = jnp.exp(-log_var)
    err_sum = jnp.zeros((OUT_PAD, 128), F32)
    off_sum = jnp.zeros((OUT_PAD, 128), F32)
    bias_sum = jnp.zeros((H, 128), F32)
    for i in range(ROWS // CHUNK):
        src, start = (mine, CHUNK * i) if i < 3 else (other, CHUNK * i - 768)
        here = slice(CHUNK * i, CHUNK * i + CHUNK)
        count = counts[0:1, here]
        pre_act = (
            lax.dot_general(w1t[...], xs[here, :], (((1,), (1,)), ((), ())), preferred_element_type=F32) + bias_h
        )
        gate = jax.nn.sigmoid(pre_act)
        hidden[:, here] = (pre_act * gate).astype(BF16)
        slope[...] = gate * (1.0 + pre_act * (1.0 - gate))
        goal = src[start : start + CHUNK, 512:896].astype(F32).T
        pred = jnp.dot(w2t[...], hidden[:, here], preferred_element_type=F32) + bias_o
        residual = pred - goal
        scaled = residual * shrink
        err = residual * scaled * count
        grad = scaled * (1.0 / ROWS)
        weighed = grad * count
        err_sum += err[:, 0:128] + err[:, 128:256]
        off_sum += weighed[:, 0:128] + weighed[:, 128:256]
        weighted[:, here] = weighed.astype(BF16)
        back = jnp.dot(w2[...], grad.astype(BF16), preferred_element_type=F32)
        grad_pre = back * slope[...] * count
        bias_sum += grad_pre[:, 0:128] + grad_pre[:, 128:256]
        pre[:, here] = grad_pre.astype(BF16)
    upper = lax.dot_general(hidden[...], weighted[...], (((1,), (1,)), ((), ())), preferred_element_type=F32)
    lower = jnp.dot(pre[...], xs[...], preferred_element_type=F32)
    bias = jnp.sum(bias_sum, axis=1, keepdims=True)
    high = bias.astype(BF16).astype(F32)
    lane = lax.broadcasted_iota(jnp.int32, (H, 128), 1)
    tail = lower[:, 384:512]
    tail = jnp.where(lane == IN - 384, high, jnp.where(lane == IN - 383, bias - high, tail))
    blocks = [upper[:, 128 * j : 128 * j + 128].astype(BF16) for j in range(3)]
    blocks += [lower[:, 128 * j : 128 * j + 128].astype(BF16) for j in range(3)]
    blocks.append(tail.astype(BF16))
    second = lax.axis_index("member_1") == 1
    for z in range(8):
        for y in range(8):
            a, b = jnp.where(second, y, z), jnp.where(second, z, y)
            at = (z * 8 + y) * 16
            for j in range(7):
                send[a, pl.ds(pl.multiple_of(b * TILE + 16 * j, 16), 16), :] = blocks[j][at : at + 16, :]
    err_col = jnp.sum(err_sum, axis=1, keepdims=True)
    off_col = jnp.sum(off_sum, axis=1, keepdims=True)
    feature = lax.broadcasted_iota(jnp.int32, (OUT_PAD, 1), 0)
    real = feature < OUT
    loss = 0.5 * jnp.sum(jnp.where(real, err_col + ROWS * log_var, 0.0), axis=0, keepdims=True) * (1.0 / ROWS)
    noise_col = jnp.where(feature == OUT, loss, 0.5 * (ROWS - err_col) * (1.0 / ROWS))
    vectors = jnp.zeros((128, 128), F32)
    lane = lax.broadcasted_iota(jnp.int32, (128, 128), 1)
    for t in range(3):
        for i, col in enumerate((off_col, noise_col)):
            part = col[128 * t : 128 * t + 128, :]
            high = part.astype(BF16).astype(F32)
            vectors = jnp.where(lane == 4 * t + 2 * i, high, vectors)
            vectors = jnp.where(lane == 4 * t + 2 * i + 1, part - high, vectors)
    vectors = vectors.T[0:16, :].astype(BF16)
    for a in range(8):
        send[a, 8 * TILE : 8 * TILE + 16, :] = vectors
    del goal_t, grads


def middle_body(got, send):
    for b in range(8):
        at = slice(b * TILE, b * TILE + TILE)
        send[b, 0:TILE, :] = jnp.sum(got[:, at, :].astype(F32), axis=0)
    vectors = jnp.sum(got[:, 8 * TILE : 8 * TILE + 16, :].astype(F32), axis=0)
    rows = [vectors[2 * i : 2 * i + 1, :] + vectors[2 * i + 1 : 2 * i + 2, :] for i in range(6)]
    for b in range(8):
        for i in range(6):
            send[b, TILE + i : TILE + i + 1, :] = rows[i]
        send[b, TILE + 6 : TILE + 8, :] = jnp.zeros((2, 128), F32)


def finish_body(got, lower, bias, upper, offset, noise, loss):
    total = jnp.sum(got[...], axis=0)
    for j in range(3):
        width = min(128, OUT - 128 * j)
        upper[0, :, 128 * j : 128 * j + width] = total[16 * j : 16 * j + 16, 0:width]
        offset[:, 128 * j : 128 * j + width] = total[TILE + 2 * j : TILE + 2 * j + 1, 0:width]
        noise[:, 128 * j : 128 * j + width] = total[TILE + 2 * j + 1 : TILE + 2 * j + 2, 0:width]
    for j in range(4):
        width = min(128, IN - 128 * j)
        lower[0, :, 128 * j : 128 * j + width] = total[48 + 16 * j : 64 + 16 * j, 0:width]
    tail = total[96:112, :]
    bias[...] = tail[:, 9:10] + tail[:, 10:11]
    loss[...] = total[TILE + 5 : TILE + 6, OUT - 256 : OUT - 255]


def exchange(x, **kw):
    return lax.all_to_all(x, kw.pop("axes"), 0, 0, tiled=True, **kw)


def per_device(inputs, targets, bootstrap, lower_weight, lower_shift, upper_weight, upper_shift, log_var):
    both, stats = call(prepare_body, (shape(PIECE, 896, dtype=BF16), shape(16, 8, 128)), 2)(inputs, targets)
    pieces = [both]
    for d in (1, 2, 3):
        pieces.append(lax.ppermute(both, "member_0", [(i, (i + d) % 4) for i in range(4)]))
    counts = call(lambda b, r: counts_body(b, None, r), shape(8, ROWS), 1)(bootstrap)
    w1t = jnp.pad(lower_weight[0].T, ((0, 0), (0, IN_PAD - IN)))
    w2 = jnp.pad(upper_weight[0], ((0, 0), (0, OUT_PAD - OUT)))
    w2t = w2.T
    cols_h = lower_shift.T
    cols_o = jnp.pad(jnp.stack([upper_shift[0], log_var[0]], axis=1), ((0, OUT_PAD - OUT), (0, 0)))
    stats = exchange(stats, axes=("dp_1", "member_1"))
    stats = call(merge_body, shape(32, 8, 128), 1)(stats)
    stats = exchange(stats, axes=("dp_0", "member_0"))
    mine = jnp.concatenate(pieces, axis=0)
    other = lax.ppermute(mine, "member_1", [(0, 1), (1, 0)])
    send = call(
        step_body,
        shape(8, 8 * TILE + 16, 128, dtype=BF16),
        9,
        scratch=(
            pltpu.VMEM((ROWS, IN_PAD), BF16),
            pltpu.VMEM((H, ROWS), BF16),
            pltpu.VMEM((H, CHUNK), F32),
            pltpu.VMEM((8, 128), BF16),
            pltpu.VMEM((OUT_PAD, ROWS), BF16),
            pltpu.VMEM((H, ROWS), BF16),
            pltpu.VMEM((8, 128), F32),
        ),
        flops=7_000_000_000,
        moved=10_000_000,
    )(mine, other, stats, counts, w1t, w2, w2t, cols_h, cols_o)
    got = exchange(send, axes=ALL, axis_index_groups=FIRST)
    send = call(middle_body, shape(8, TILE + 8, 128), 1)(got)
    got = exchange(send, axes=ALL, axis_index_groups=SECOND)
    lower_grad, bias_grad, upper_grad, offset_grad, noise_grad, member_loss = call(
        finish_body,
        (shape(1, 16, IN), shape(16, 1), shape(1, 16, OUT), shape(1, OUT), shape(1, OUT), shape(1, 1)),
        1,
    )(got)
    return (lower_grad, bias_grad.reshape(1, 16), upper_grad, offset_grad, noise_grad, member_loss.reshape(1))


def solution(mesh):
    finer = Mesh(mesh.devices.reshape(8, 8, 4, 2), ALL)
    return jax.shard_map(
        per_device,
        mesh=finer,
        in_specs=(
            P(ALL, None),
            P(ALL, None),
            P(MEMBER, DP),
            P(MEMBER, None, None),
            P(MEMBER, None),
            P(MEMBER, None, None),
            P(MEMBER, None),
            P(MEMBER, None),
        ),
        out_specs=(
            P(MEMBER, DP, None),
            P(MEMBER, DP),
            P(MEMBER, DP, None),
            P(MEMBER, None),
            P(MEMBER, None),
            P(MEMBER),
        ),
        check_vma=False,
    )
```

```python
import jax
import jax.numpy as jnp
from jax import lax
from jax.experimental import pallas as pl
from jax.experimental.pallas import tpu as pltpu
from jax.sharding import Mesh
from jax.sharding import PartitionSpec as P


IN, OUT, H = 393, 377, 1024
IN_PAD, OUT_PAD = 512, 384
ROWS = 1536
PIECE = 192
TOTAL = 98304
CHUNK = 256
TILE = 96
DP = ("dp_0", "dp_1")
MEMBER = ("member_0", "member_1")
ALL = ("dp_0", "dp_1", "member_0", "member_1")
BF16, F32 = jnp.bfloat16, jnp.float32


def groups_by(key):
    found = {}
    for z in range(8):
        for y in range(8):
            for x in range(4):
                for c in range(2):
                    found.setdefault(key(z, y, x, c), []).append(((z * 8 + y) * 4 + x) * 2 + c)
    return list(found.values())


FIRST = groups_by(lambda z, y, x, c: (c, x, y) if c == 0 else (c, x, z))
SECOND = groups_by(lambda z, y, x, c: (c, x, z) if c == 0 else (c, x, y))


def call(body, outs, n_in, scratch=(), flops=0, moved=0, limit=8, far=()):
    return pl.pallas_call(
        body,
        out_shape=outs,
        in_specs=[pl.BlockSpec(memory_space=pltpu.HBM if i in far else pltpu.VMEM) for i in range(n_in)],
        out_specs=jax.tree.map(lambda _: pl.BlockSpec(memory_space=pltpu.VMEM), outs),
        scratch_shapes=list(scratch),
        compiler_params=pltpu.CompilerParams(vmem_limit_bytes=limit * 1024 * 1024),
        cost_estimate=pl.CostEstimate(flops=flops, bytes_accessed=moved, transcendentals=0),
    )


def shape(*dims, dtype=F32):
    return jax.ShapeDtypeStruct(dims, dtype)


def prepare_body(inputs_hbm, targets_hbm, both, stats, inputs, targets, arrived):
    copies = [
        pltpu.make_async_copy(inputs_hbm, inputs, arrived.at[0]),
        pltpu.make_async_copy(targets_hbm, targets, arrived.at[1]),
    ]
    for copy in copies:
        copy.start()
    both[:, 384:512] = jnp.zeros((PIECE, 128), BF16)
    both[:, 768:896] = jnp.zeros((PIECE, 128), BF16)
    stats[...] = jnp.zeros(stats.shape, F32)
    copies[0].wait()
    both[:, 0:IN] = inputs[...]
    for t in range(4):
        width = min(128, IN - 128 * t)
        v = inputs[:, 128 * t : 128 * t + width].astype(F32)
        mean = jnp.sum(v, axis=0, keepdims=True) * (1.0 / PIECE)
        centred = v - mean
        square = jnp.sum(centred * centred, axis=0, keepdims=True)
        for i in range(stats.shape[0]):
            stats[i, t : t + 1, 0:width] = mean
            stats[i, 4 + t : 5 + t, 0:width] = square
    copies[1].wait()
    both[:, 512 : 512 + OUT] = targets[...]


def merged(stats, rows_each):
    means, squares = stats[:, 0:4, :], stats[:, 4:8, :]
    mean = jnp.sum(means, axis=0) * (1.0 / stats.shape[0])
    away = means - mean[None]
    return mean, jnp.sum(squares, axis=0) + rows_each * jnp.sum(away * away, axis=0)


def merge_body(stats, out):
    mean, square = merged(stats[...], float(PIECE))
    for i in range(out.shape[0]):
        out[i, 0:4, :] = mean
        out[i, 4:8, :] = square


def stack_body(*refs):
    for i in range(4):
        refs[4][PIECE * i : PIECE * i + PIECE, :] = refs[i][...]


def counts_body(bootstrap, counts):
    x, c = lax.axis_index("member_0"), lax.axis_index("member_1")
    shift = []
    for p in range(8):
        core = c if p < 4 else 1 - c
        member = lax.rem(x + 4 - p % 4, 4) * 2 + core
        shift.append((member - p) * PIECE)
    picks = bootstrap[...]
    for k in range(ROWS // 128):
        first, last = 128 * k // PIECE, (128 * k + 127) // PIECE
        place = lax.broadcasted_iota(jnp.int32, (128, 1), 0) + 128 * k
        row_id = place + jnp.where(place < PIECE * (first + 1), shift[first], shift[last])
        hits = (picks == row_id).astype(F32)
        total = jnp.sum(hits, axis=1, keepdims=True)
        counts[:, 128 * k : 128 * k + 128] = jnp.broadcast_to(total, (128, 128)).T[0:8, :]


def lower_body(w1, w1t, spare):
    spare[...] = jnp.zeros(spare.shape, F32)
    spare[0 : IN - 384, :] = w1[0, 384:IN, :].astype(F32)
    w1t[:, 0:384] = w1[0, 0:384, :].T
    w1t[:, 384:512] = spare[...].astype(BF16).T


def as_column(row, n):
    return jnp.concatenate(
        [jnp.broadcast_to(row[:, 128 * t : 128 * t + 128], (128, 128)).T for t in range(n // 128)], axis=0
    )


def twice(x):
    return jnp.concatenate([x, x], axis=1)


def folded(x):
    return x[:, 0:128] + x[:, 128:256]


def step_body(
    mine, other_hbm, stats, counts, w1t, w2_hbm, b1, b2, lv, send, xs, hidden, slope, weighted, pre, odd, other, w2_in, w2, w2t, row, arrived
):
    copies = [
        pltpu.make_async_copy(w2_hbm, w2_in, arrived.at[0]),
        pltpu.make_async_copy(other_hbm, other, arrived.at[1]),
    ]
    for copy in copies:
        copy.start()
    row[...] = jnp.zeros(row.shape, F32)
    row[0:1, 0:OUT] = b2[...]
    row[1:2, 0:OUT] = lv[...]
    bias_h, bias_o = as_column(b1[...], H), as_column(row[0:1, :], OUT_PAD)
    mean, square = merged(stats[...], float(PIECE * 16))
    scale = 1.0 / jnp.sqrt(square * (1.0 / TOTAL) + 1e-06)

    def rescale(half, src):
        for t in range(4):
            lanes = slice(128 * t, 128 * t + 128)
            v = (src[:, lanes].astype(F32) - mean[t : t + 1, :]) * scale[t : t + 1, :]
            xs[768 * half : 768 * half + 768, lanes] = v.astype(BF16)

    rescale(0, mine)
    log_var = as_column(row[1:2, :], OUT_PAD)
    shrink = twice(jnp.exp(-log_var))
    err_sum = jnp.zeros((OUT_PAD, 128), F32)
    off_sum = jnp.zeros((OUT_PAD, 128), F32)
    bias_sum = jnp.zeros((H, 128), F32)
    for i in range(ROWS // CHUNK):
        src, start = (mine, CHUNK * i) if i < 3 else (other, CHUNK * i - 768)
        if i == 3:
            copies[1].wait()
            rescale(1, other)
        here = slice(CHUNK * i, CHUNK * i + CHUNK)
        count = counts[0:1, here]
        pre_act = lax.dot_general(w1t[...], xs[here, :], (((1,), (1,)), ((), ())), preferred_element_type=F32)
        pre_act = pre_act + twice(bias_h)
        gate = jax.nn.sigmoid(pre_act)
        hidden[:, here] = (pre_act * gate).astype(BF16)
        slope[...] = gate * (1.0 + pre_act * (1.0 - gate))
        if i == 0:
            copies[0].wait()
            w2[:, 256:384] = jnp.zeros((H, 128), BF16)
            w2[:, 0:OUT] = w2_in[0]
            w2t[...] = w2[...].T
        goal = src[start : start + CHUNK, 512:896].astype(F32).T
        pred = jnp.dot(w2t[...], hidden[:, here], preferred_element_type=F32) + twice(bias_o)
        residual = pred - goal
        scaled = residual * shrink
        err_sum += folded(residual * scaled * count)
        grad = scaled * (1.0 / ROWS)
        weighed = grad * count
        off_sum += folded(weighed)
        weighted[:, here] = weighed.astype(BF16)
        back = jnp.dot(w2[...], grad.astype(BF16), preferred_element_type=F32)
        grad_pre = back * slope[...] * count
        bias_sum += folded(grad_pre)
        pre[:, here] = grad_pre.astype(BF16)
    upper = lax.dot_general(hidden[...], weighted[...], (((1,), (1,)), ((), ())), preferred_element_type=F32)
    lower = jnp.dot(pre[...], xs[...], preferred_element_type=F32)
    bias = jnp.sum(bias_sum, axis=1, keepdims=True)
    high = bias.astype(BF16).astype(F32)
    lane = lax.broadcasted_iota(jnp.int32, (H, 128), 1)
    tail = lower[:, 384:512]
    filled = jnp.where(lane >= OUT - 256, pltpu.roll(tail, OUT - 256, axis=1), upper[:, 256:384])
    rest = jnp.where((lane == 12) | (lane == 13), pltpu.roll(tail, 5, axis=1), 0.0)
    rest = jnp.where(lane == 14, high, jnp.where(lane == 15, bias - high, rest))
    blocks = [upper[:, 0:128], upper[:, 128:256], filled] + [lower[:, 128 * j : 128 * j + 128] for j in range(3)]
    blocks = [block.astype(BF16) for block in blocks]
    second = lax.axis_index("member_1") == 1
    for z in range(8):
        for y in range(8):
            a, b = jnp.where(second, y, z), jnp.where(second, z, y)
            at = (z * 8 + y) * 16
            for j in range(6):
                send[a, pl.ds(pl.multiple_of(b * TILE + 16 * j, 16), 16), :] = blocks[j][at : at + 16, :]
            odd[pl.ds(pl.multiple_of(a * 128 + b * 16, 16), 16), :] = rest[at : at + 16, :]
    err_col = jnp.sum(err_sum, axis=1, keepdims=True)
    off_col = jnp.sum(off_sum, axis=1, keepdims=True)
    feature = lax.broadcasted_iota(jnp.int32, (OUT_PAD, 1), 0)
    real = feature < OUT
    loss = 0.5 * jnp.sum(jnp.where(real, err_col + ROWS * log_var[:, 0:1], 0.0), axis=0, keepdims=True) * (1.0 / ROWS)
    noise_col = jnp.where(feature == OUT, loss, 0.5 * (ROWS - err_col) * (1.0 / ROWS))
    vectors = jnp.zeros((128, 128), F32)
    lane = lax.broadcasted_iota(jnp.int32, (128, 128), 1)
    for t in range(3):
        for i, col in enumerate((off_col, noise_col)):
            part = col[128 * t : 128 * t + 128, :]
            high = part.astype(BF16).astype(F32)
            vectors = jnp.where(lane == 4 * t + 2 * i, high, vectors)
            vectors = jnp.where(lane == 4 * t + 2 * i + 1, part - high, vectors)
    vectors = vectors.T[0:16, :]
    for a in range(8):
        send[a, 8 * TILE : 8 * TILE + 16, :] = (vectors + odd[128 * a : 128 * a + 128, :].T[0:16, :]).astype(BF16)


def middle_body(got, send):
    for b in range(8):
        at = slice(b * TILE, b * TILE + TILE)
        send[b, 0:TILE, :] = jnp.sum(got[:, at, :].astype(F32), axis=0)
    last = jnp.sum(got[:, 8 * TILE : 8 * TILE + 16, :].astype(F32), axis=0)
    rows = [last[2 * i : 2 * i + 1, :] + last[2 * i + 1 : 2 * i + 2, :] for i in range(6)]
    bias = last[14:15, :] + last[15:16, :]
    turned = jnp.concatenate([last, jnp.zeros((112, 128), F32)], axis=0).T
    for b in range(8):
        send[b, TILE : TILE + 16, :] = turned[16 * b : 16 * b + 16, :]
        for i in range(6):
            send[b, TILE + 16 + i : TILE + 17 + i, :] = rows[i]
        send[b, TILE + 22 : TILE + 23, :] = pltpu.roll(bias, (128 - 16 * b) % 128, axis=1)
        send[b, TILE + 23 : TILE + 24, :] = jnp.zeros((1, 128), F32)


def finish_body(got, lower, bias, upper, offset, noise, loss):
    total = jnp.sum(got[...], axis=0)
    at = TILE + 16
    for j in range(3):
        width = min(128, OUT - 128 * j)
        upper[0, :, 128 * j : 128 * j + width] = total[16 * j : 16 * j + 16, 0:width]
        lower[0, :, 128 * j : 128 * j + 128] = total[48 + 16 * j : 64 + 16 * j, :]
        offset[:, 128 * j : 128 * j + width] = total[at + 2 * j : at + 2 * j + 1, 0:width]
        noise[:, 128 * j : 128 * j + width] = total[at + 2 * j + 1 : at + 2 * j + 2, 0:width]
    lower[0, :, 384:391] = total[32:48, OUT - 256 : 128]
    lower[0, :, 391:393] = total[TILE : TILE + 16, 12:14]
    bias[...] = total[at + 6 : at + 7, 0:16]
    loss[...] = total[at + 5 : at + 6, OUT - 256 : OUT - 255]


def exchange(x, **kw):
    return lax.all_to_all(x, kw.pop("axes"), 0, 0, tiled=True, **kw)


def per_device(inputs, targets, bootstrap, lower_weight, lower_shift, upper_weight, upper_shift, log_var):
    both, stats = call(
        prepare_body,
        (shape(PIECE, 896, dtype=BF16), shape(16, 8, 128)),
        2,
        scratch=(pltpu.VMEM((PIECE, IN), BF16), pltpu.VMEM((PIECE, OUT), BF16), pltpu.SemaphoreType.DMA((2,))),
        far=(0, 1),
    )(inputs, targets)
    pieces = [both]
    for d in (1, 2, 3):
        pieces.append(lax.ppermute(both, "member_0", [(i, (i + d) % 4) for i in range(4)]))
    stats = exchange(stats, axes=("dp_1", "member_1"))
    *pieces, stats = lax.optimization_barrier((*pieces, stats))
    stats = call(merge_body, shape(32, 8, 128), 1)(stats)
    stats = exchange(stats, axes=("dp_0", "member_0"))
    mine = call(stack_body, shape(4 * PIECE, 896, dtype=BF16), 4)(*pieces)
    other = lax.ppermute(mine, "member_1", [(0, 1), (1, 0)])
    counts = call(counts_body, shape(8, ROWS), 1, flops=5_000_000)(bootstrap)
    w1t = call(lower_body, shape(H, IN_PAD, dtype=BF16), 1, scratch=(pltpu.VMEM((128, H), F32),))(lower_weight)
    send = call(
        step_body,
        shape(8, 8 * TILE + 16, 128, dtype=BF16),
        9,
        scratch=(
            pltpu.VMEM((ROWS, IN_PAD), BF16),
            pltpu.VMEM((H, ROWS), BF16),
            pltpu.VMEM((H, CHUNK), F32),
            pltpu.VMEM((OUT_PAD, ROWS), BF16),
            pltpu.VMEM((H, ROWS), BF16),
            pltpu.VMEM((H, 128), F32),
            pltpu.VMEM((4 * PIECE, 896), BF16),
            pltpu.VMEM((1, H, OUT), BF16),
            pltpu.VMEM((H, OUT_PAD), BF16),
            pltpu.VMEM((OUT_PAD, H), BF16),
            pltpu.VMEM((8, OUT_PAD), F32),
            pltpu.SemaphoreType.DMA((2,)),
        ),
        far=(1, 5),
        flops=7_000_000_000,
        moved=10_000_000,
        limit=24,
    )(mine, other, stats, counts, w1t, upper_weight, lower_shift, upper_shift, log_var)
    got = exchange(send, axes=ALL, axis_index_groups=FIRST)
    send = call(middle_body, shape(8, TILE + 24, 128), 1)(got)
    got = exchange(send, axes=ALL, axis_index_groups=SECOND)
    lower_grad, bias_grad, upper_grad, offset_grad, noise_grad, member_loss = call(
        finish_body,
        (shape(1, 16, IN), shape(1, 16), shape(1, 16, OUT), shape(1, OUT), shape(1, OUT), shape(1, 1)),
        1,
    )(got)
    return (lower_grad, bias_grad, upper_grad, offset_grad, noise_grad, member_loss.reshape(1))


def solution(mesh):
    finer = Mesh(mesh.devices.reshape(8, 8, 4, 2), ALL)
    return jax.shard_map(
        per_device,
        mesh=finer,
        in_specs=(
            P(ALL, None),
            P(ALL, None),
            P(MEMBER, DP),
            P(MEMBER, None, None),
            P(MEMBER, None),
            P(MEMBER, None, None),
            P(MEMBER, None),
            P(MEMBER, None),
        ),
        out_specs=(
            P(MEMBER, DP, None),
            P(MEMBER, DP),
            P(MEMBER, DP, None),
            P(MEMBER, None),
            P(MEMBER, None),
            P(MEMBER),
        ),
        check_vma=False,
    )
```

```python
import jax
import jax.numpy as jnp
from jax import lax
from jax.experimental import pallas as pl
from jax.experimental.pallas import tpu as pltpu
from jax.sharding import Mesh
from jax.sharding import PartitionSpec as P


IN, OUT, H = 393, 377, 1024
IN_PAD, OUT_PAD = 512, 384
ROWS = 1536
PIECE = 192
TOTAL = 98304
CHUNK = 256
BLOCK = 512
TILE = 96
DP = ("dp_0", "dp_1")
MEMBER = ("member_0", "member_1")
ALL = ("dp_0", "dp_1", "member_0", "member_1")
BF16, F32 = jnp.bfloat16, jnp.float32


def groups_by(key):
    found = {}
    for z in range(8):
        for y in range(8):
            for x in range(4):
                for c in range(2):
                    found.setdefault(key(z, y, x, c), []).append(((z * 8 + y) * 4 + x) * 2 + c)
    return list(found.values())


FIRST = groups_by(lambda z, y, x, c: (c, x, y) if c == 0 else (c, x, z))
SECOND = groups_by(lambda z, y, x, c: (c, x, z) if c == 0 else (c, x, y))


def call(body, outs, n_in, scratch=(), flops=0, moved=0, limit=8, far=()):
    return pl.pallas_call(
        body,
        out_shape=outs,
        in_specs=[pl.BlockSpec(memory_space=pltpu.HBM if i in far else pltpu.VMEM) for i in range(n_in)],
        out_specs=jax.tree.map(lambda _: pl.BlockSpec(memory_space=pltpu.VMEM), outs),
        scratch_shapes=list(scratch),
        compiler_params=pltpu.CompilerParams(vmem_limit_bytes=limit * 1024 * 1024),
        cost_estimate=pl.CostEstimate(flops=flops, bytes_accessed=moved, transcendentals=0),
    )


def shape(*dims, dtype=F32):
    return jax.ShapeDtypeStruct(dims, dtype)


def prepare_body(inputs_hbm, targets_hbm, both, stats, inputs, targets, arrived):
    copies = [
        pltpu.make_async_copy(inputs_hbm, inputs, arrived.at[0]),
        pltpu.make_async_copy(targets_hbm, targets, arrived.at[1]),
    ]
    for copy in copies:
        copy.start()
    both[:, 384:512] = jnp.zeros((PIECE, 128), BF16)
    both[:, 768:896] = jnp.zeros((PIECE, 128), BF16)
    stats[...] = jnp.zeros(stats.shape, F32)
    copies[0].wait()
    both[:, 0:IN] = inputs[...]
    for t in range(4):
        width = min(128, IN - 128 * t)
        v = inputs[:, 128 * t : 128 * t + width].astype(F32)
        mean = jnp.sum(v, axis=0, keepdims=True) * (1.0 / PIECE)
        centred = v - mean
        square = jnp.sum(centred * centred, axis=0, keepdims=True)
        for i in range(stats.shape[0]):
            stats[i, t : t + 1, 0:width] = mean
            stats[i, 4 + t : 5 + t, 0:width] = square
    copies[1].wait()
    both[:, 512 : 512 + OUT] = targets[...]


def merged(stats, rows_each):
    means, squares = stats[:, 0:4, :], stats[:, 4:8, :]
    mean = jnp.sum(means, axis=0) * (1.0 / stats.shape[0])
    away = means - mean[None]
    return mean, jnp.sum(squares, axis=0) + rows_each * jnp.sum(away * away, axis=0)


def merge_body(stats, out):
    mean, square = merged(stats[...], float(PIECE))
    for i in range(out.shape[0]):
        out[i, 0:4, :] = mean
        out[i, 4:8, :] = square


def stack_body(*refs):
    for i in range(4):
        refs[4][PIECE * i : PIECE * i + PIECE, :] = refs[i][...]


def counts_body(bootstrap, counts):
    x, c = lax.axis_index("member_0"), lax.axis_index("member_1")
    shift = []
    for p in range(8):
        core = c if p < 4 else 1 - c
        member = lax.rem(x + 4 - p % 4, 4) * 2 + core
        shift.append((member - p) * PIECE)
    picks = bootstrap[...]
    for k in range(ROWS // 128):
        first, last = 128 * k // PIECE, (128 * k + 127) // PIECE
        place = lax.broadcasted_iota(jnp.int32, (128, 1), 0) + 128 * k
        row_id = place + jnp.where(place < PIECE * (first + 1), shift[first], shift[last])
        hits = (picks == row_id).astype(F32)
        total = jnp.sum(hits, axis=1, keepdims=True)
        counts[:, 128 * k : 128 * k + 128] = jnp.broadcast_to(total, (128, 128)).T[0:8, :]


def lower_body(w1, b1, w1t, spare):
    spare[...] = jnp.zeros(spare.shape, F32)
    spare[0 : IN - 384, :] = w1[0, 384:IN, :].astype(F32)
    left = b1[...]
    for i in range(3):
        part = left.astype(BF16).astype(F32)
        spare[IN - 384 + i : IN - 383 + i, :] = part
        left = left - part
    for t in range(3):
        w1t[:, 128 * t : 128 * t + 128] = (w1[0, 128 * t : 128 * t + 128, :].astype(F32) * 0.5).astype(BF16).T
    w1t[:, 384:512] = (spare[...] * 0.5).astype(BF16).T


def as_column(row, n):
    return jnp.concatenate(
        [jnp.broadcast_to(row[:, 128 * t : 128 * t + 128], (128, 128)).T for t in range(n // 128)], axis=0
    )


def twice(x):
    return jnp.concatenate([x, x], axis=1)


def folded(x):
    return x[:, 0:128] + x[:, 128:256]


def step_body(
    mine, other_hbm, stats, counts, w1t, w2_in, b2, lv, send, xs, hidden, slope, weighted, pre, odd, other, w2, w2t, row, arrived
):
    arrival = pltpu.make_async_copy(other_hbm, other, arrived)
    arrival.start()
    w2[:, 256:384] = jnp.zeros((H, 128), BF16)
    w2[:, 0:OUT] = w2_in[0]
    w2t[...] = w2[...].T
    row[...] = jnp.zeros(row.shape, F32)
    row[0:1, 0:OUT] = b2[...]
    row[1:2, 0:OUT] = lv[...]
    bias_o = as_column(row[0:1, :], OUT_PAD)
    mean, square = merged(stats[...], float(PIECE * 16))
    scale = 1.0 / jnp.sqrt(square * (1.0 / TOTAL) + 1e-06)

    def rescale(half, src):
        for t in range(4):
            lanes = slice(128 * t, 128 * t + 128)
            v = (src[:, lanes].astype(F32) - mean[t : t + 1, :]) * scale[t : t + 1, :]
            if t == 3:
                lane = lax.broadcasted_iota(jnp.int32, v.shape, 1)
                v = jnp.where((lane >= IN - 384) & (lane < IN - 381), 1.0, v)
            xs[768 * half : 768 * half + 768, lanes] = v.astype(BF16)

    rescale(0, mine)
    log_var = as_column(row[1:2, :], OUT_PAD)
    shrink = twice(jnp.exp(-log_var))
    err_sum = jnp.zeros((OUT_PAD, 128), F32)
    off_sum = jnp.zeros((OUT_PAD, 128), F32)
    for i in range(ROWS // CHUNK):
        src, start = (mine, CHUNK * i) if i < 3 else (other, CHUNK * i - 768)
        if i == 3:
            arrival.wait()
            rescale(1, other)
        here = slice(CHUNK * i, CHUNK * i + CHUNK)
        count = counts[0:1, here]
        for h in range(0, H, BLOCK):
            block = slice(h, h + BLOCK)
            halved = lax.dot_general(
                w1t[block, :], xs[here, :], (((1,), (1,)), ((), ())), preferred_element_type=F32
            )
            twofold = jnp.tanh(halved) + 1.0
            value = halved * twofold
            gate = 0.5 * twofold
            hidden[block, here] = value.astype(BF16)
            slope[block, :] = (gate + value) - value * gate
        goal = src[start : start + CHUNK, 512:896].astype(F32).T
        pred = jnp.dot(w2t[...], hidden[:, here], preferred_element_type=F32) + twice(bias_o)
        residual = pred - goal
        scaled = residual * shrink
        err_sum += folded(residual * scaled * count)
        grad = scaled * (1.0 / ROWS)
        weighed = grad * count
        off_sum += folded(weighed)
        weighted[:, here] = weighed.astype(BF16)
        for h in range(0, H, BLOCK):
            block = slice(h, h + BLOCK)
            back = jnp.dot(w2[block, :], weighted[:, here], preferred_element_type=F32)
            pre[block, here] = (back * slope[block, :]).astype(BF16)
    upper = lax.dot_general(hidden[...], weighted[...], (((1,), (1,)), ((), ())), preferred_element_type=F32)
    lower = jnp.dot(pre[...], xs[...], preferred_element_type=F32)
    lane = lax.broadcasted_iota(jnp.int32, (H, 128), 1)
    tail = lower[:, 384:512]
    filled = jnp.where(lane >= OUT - 256, pltpu.roll(tail, OUT - 256, axis=1), upper[:, 256:384])
    bias = pltpu.roll(tail, 6, axis=1)
    rest = jnp.where((lane >= 12) & (lane < 15), pltpu.roll(tail, 5, axis=1), 0.0)
    rest = jnp.where(lane == 15, bias - bias.astype(BF16).astype(F32), rest)
    blocks = [upper[:, 0:128], upper[:, 128:256], filled] + [lower[:, 128 * j : 128 * j + 128] for j in range(3)]
    blocks = [block.astype(BF16) for block in blocks]
    second = lax.axis_index("member_1") == 1
    for z in range(8):
        for y in range(8):
            a, b = jnp.where(second, y, z), jnp.where(second, z, y)
            at = (z * 8 + y) * 16
            for j in range(6):
                send[a, pl.ds(pl.multiple_of(b * TILE + 16 * j, 16), 16), :] = blocks[j][at : at + 16, :]
            odd[pl.ds(pl.multiple_of(a * 128 + b * 16, 16), 16), :] = rest[at : at + 16, :]
    err_col = jnp.sum(err_sum, axis=1, keepdims=True)
    off_col = jnp.sum(off_sum, axis=1, keepdims=True)
    feature = lax.broadcasted_iota(jnp.int32, (OUT_PAD, 1), 0)
    real = feature < OUT
    loss = 0.5 * jnp.sum(jnp.where(real, err_col + ROWS * log_var[:, 0:1], 0.0), axis=0, keepdims=True) * (1.0 / ROWS)
    noise_col = jnp.where(feature == OUT, loss, 0.5 * (ROWS - err_col) * (1.0 / ROWS))
    vectors = jnp.zeros((128, 128), F32)
    lane = lax.broadcasted_iota(jnp.int32, (128, 128), 1)
    for t in range(3):
        for i, col in enumerate((off_col, noise_col)):
            part = col[128 * t : 128 * t + 128, :]
            high = part.astype(BF16).astype(F32)
            vectors = jnp.where(lane == 4 * t + 2 * i, high, vectors)
            vectors = jnp.where(lane == 4 * t + 2 * i + 1, part - high, vectors)
    vectors = vectors.T[0:16, :]
    for a in range(8):
        send[a, 8 * TILE : 8 * TILE + 16, :] = (vectors + odd[128 * a : 128 * a + 128, :].T[0:16, :]).astype(BF16)


def middle_body(got, send):
    for b in range(8):
        at = slice(b * TILE, b * TILE + TILE)
        send[b, 0:TILE, :] = jnp.sum(got[:, at, :].astype(F32), axis=0)
    last = jnp.sum(got[:, 8 * TILE : 8 * TILE + 16, :].astype(F32), axis=0)
    rows = [last[2 * i : 2 * i + 1, :] + last[2 * i + 1 : 2 * i + 2, :] for i in range(6)]
    bias = last[14:15, :] + last[15:16, :]
    turned = jnp.concatenate([last, jnp.zeros((112, 128), F32)], axis=0).T
    for b in range(8):
        send[b, TILE : TILE + 16, :] = turned[16 * b : 16 * b + 16, :]
        for i in range(6):
            send[b, TILE + 16 + i : TILE + 17 + i, :] = rows[i]
        send[b, TILE + 22 : TILE + 23, :] = pltpu.roll(bias, (128 - 16 * b) % 128, axis=1)
        send[b, TILE + 23 : TILE + 24, :] = jnp.zeros((1, 128), F32)


def finish_body(got, lower, bias, upper, offset, noise, loss):
    total = jnp.sum(got[...], axis=0)
    at = TILE + 16
    for j in range(3):
        width = min(128, OUT - 128 * j)
        upper[0, :, 128 * j : 128 * j + width] = total[16 * j : 16 * j + 16, 0:width]
        lower[0, :, 128 * j : 128 * j + 128] = total[48 + 16 * j : 64 + 16 * j, :]
        offset[:, 128 * j : 128 * j + width] = total[at + 2 * j : at + 2 * j + 1, 0:width]
        noise[:, 128 * j : 128 * j + width] = total[at + 2 * j + 1 : at + 2 * j + 2, 0:width]
    lower[0, :, 384:391] = total[32:48, OUT - 256 : 128]
    lower[0, :, 391:393] = total[TILE : TILE + 16, 12:14]
    bias[...] = total[at + 6 : at + 7, 0:16]
    loss[...] = total[at + 5 : at + 6, OUT - 256 : OUT - 255]


def exchange(x, **kw):
    return lax.all_to_all(x, kw.pop("axes"), 0, 0, tiled=True, **kw)


def per_device(inputs, targets, bootstrap, lower_weight, lower_shift, upper_weight, upper_shift, log_var):
    both, stats = call(
        prepare_body,
        (shape(PIECE, 896, dtype=BF16), shape(16, 8, 128)),
        2,
        scratch=(pltpu.VMEM((PIECE, IN), BF16), pltpu.VMEM((PIECE, OUT), BF16), pltpu.SemaphoreType.DMA((2,))),
        far=(0, 1),
    )(inputs, targets)
    pieces = [both]
    for d in (1, 2, 3):
        pieces.append(lax.ppermute(both, "member_0", [(i, (i + d) % 4) for i in range(4)]))
    stats = exchange(stats, axes=("dp_1", "member_1"))
    *pieces, stats = lax.optimization_barrier((*pieces, stats))
    stats = call(merge_body, shape(32, 8, 128), 1)(stats)
    stats = exchange(stats, axes=("dp_0", "member_0"))
    mine = call(stack_body, shape(4 * PIECE, 896, dtype=BF16), 4)(*pieces)
    other = lax.ppermute(mine, "member_1", [(0, 1), (1, 0)])
    counts = call(counts_body, shape(8, ROWS), 1, flops=5_000_000)(bootstrap)
    w1t = call(lower_body, shape(H, IN_PAD, dtype=BF16), 2, scratch=(pltpu.VMEM((128, H), F32),))(
        lower_weight, lower_shift
    )
    send = call(
        step_body,
        shape(8, 8 * TILE + 16, 128, dtype=BF16),
        8,
        scratch=(
            pltpu.VMEM((ROWS, IN_PAD), BF16),
            pltpu.VMEM((H, ROWS), BF16),
            pltpu.VMEM((H, CHUNK), F32),
            pltpu.VMEM((OUT_PAD, ROWS), BF16),
            pltpu.VMEM((H, ROWS), BF16),
            pltpu.VMEM((H, 128), F32),
            pltpu.VMEM((4 * PIECE, 896), BF16),
            pltpu.VMEM((H, OUT_PAD), BF16),
            pltpu.VMEM((OUT_PAD, H), BF16),
            pltpu.VMEM((8, OUT_PAD), F32),
            pltpu.SemaphoreType.DMA,
        ),
        far=(1,),
        flops=7_000_000_000,
        moved=10_000_000,
        limit=24,
    )(mine, other, stats, counts, w1t, upper_weight, upper_shift, log_var)
    got = exchange(send, axes=ALL, axis_index_groups=FIRST)
    send = call(middle_body, shape(8, TILE + 24, 128), 1)(got)
    got = exchange(send, axes=ALL, axis_index_groups=SECOND)
    lower_grad, bias_grad, upper_grad, offset_grad, noise_grad, member_loss = call(
        finish_body,
        (shape(1, 16, IN), shape(1, 16), shape(1, 16, OUT), shape(1, OUT), shape(1, OUT), shape(1, 1)),
        1,
    )(got)
    return (lower_grad, bias_grad, upper_grad, offset_grad, noise_grad, member_loss.reshape(1))


def solution(mesh):
    finer = Mesh(mesh.devices.reshape(8, 8, 4, 2), ALL)
    return jax.shard_map(
        per_device,
        mesh=finer,
        in_specs=(
            P(ALL, None),
            P(ALL, None),
            P(MEMBER, DP),
            P(MEMBER, None, None),
            P(MEMBER, None),
            P(MEMBER, None, None),
            P(MEMBER, None),
            P(MEMBER, None),
        ),
        out_specs=(
            P(MEMBER, DP, None),
            P(MEMBER, DP),
            P(MEMBER, DP, None),
            P(MEMBER, None),
            P(MEMBER, None),
            P(MEMBER),
        ),
        check_vma=False,
    )
```

```python
import jax
import jax.numpy as jnp
from jax import lax
from jax.experimental import pallas as pl
from jax.experimental.pallas import tpu as pltpu
from jax.sharding import Mesh
from jax.sharding import PartitionSpec as P


IN, OUT, H = 393, 377, 1024
IN_PAD, OUT_PAD = 512, 384
ROWS = 1536
PIECE = 192
TOTAL = 98304
CHUNK = 256
BLOCK = 512
ORDER = (0, 1, 3, 2)
NEAR = 3 * PIECE
TILE = 96
DP = ("dp_0", "dp_1")
MEMBER = ("member_0", "member_1")
ALL = ("dp_0", "dp_1", "member_0", "member_1")
BF16, F32 = jnp.bfloat16, jnp.float32


def groups_by(key):
    found = {}
    for z in range(8):
        for y in range(8):
            for x in range(4):
                for c in range(2):
                    found.setdefault(key(z, y, x, c), []).append(((z * 8 + y) * 4 + x) * 2 + c)
    return list(found.values())


FIRST = groups_by(lambda z, y, x, c: (c, x, y) if c == 0 else (c, x, z))
SECOND = groups_by(lambda z, y, x, c: (c, x, z) if c == 0 else (c, x, y))


def call(body, outs, n_in, scratch=(), flops=0, moved=0, limit=8, far=()):
    return pl.pallas_call(
        body,
        out_shape=outs,
        in_specs=[pl.BlockSpec(memory_space=pltpu.HBM if i in far else pltpu.VMEM) for i in range(n_in)],
        out_specs=jax.tree.map(lambda _: pl.BlockSpec(memory_space=pltpu.VMEM), outs),
        scratch_shapes=list(scratch),
        compiler_params=pltpu.CompilerParams(vmem_limit_bytes=limit * 1024 * 1024),
        cost_estimate=pl.CostEstimate(flops=flops, bytes_accessed=moved, transcendentals=0),
    )


def shape(*dims, dtype=F32):
    return jax.ShapeDtypeStruct(dims, dtype)


def prepare_body(inputs_hbm, targets_hbm, both, stats, inputs, targets, arrived):
    copies = [
        pltpu.make_async_copy(inputs_hbm, inputs, arrived.at[0]),
        pltpu.make_async_copy(targets_hbm, targets, arrived.at[1]),
    ]
    for copy in copies:
        copy.start()
    both[:, 384:512] = jnp.zeros((PIECE, 128), BF16)
    both[:, 768:896] = jnp.zeros((PIECE, 128), BF16)
    stats[...] = jnp.zeros(stats.shape, F32)
    copies[0].wait()
    both[:, 0:IN] = inputs[...]
    for t in range(4):
        width = min(128, IN - 128 * t)
        v = inputs[:, 128 * t : 128 * t + width].astype(F32)
        mean = jnp.sum(v, axis=0, keepdims=True) * (1.0 / PIECE)
        centred = v - mean
        square = jnp.sum(centred * centred, axis=0, keepdims=True)
        for i in range(stats.shape[0]):
            stats[i, t : t + 1, 0:width] = mean
            stats[i, 4 + t : 5 + t, 0:width] = square
    copies[1].wait()
    both[:, 512 : 512 + OUT] = targets[...]


def merged(stats, rows_each):
    means, squares = stats[:, 0:4, :], stats[:, 4:8, :]
    mean = jnp.sum(means, axis=0) * (1.0 / stats.shape[0])
    away = means - mean[None]
    return mean, jnp.sum(squares, axis=0) + rows_each * jnp.sum(away * away, axis=0)


def merge_body(stats, out):
    mean, square = merged(stats[...], float(PIECE))
    for i in range(out.shape[0]):
        out[i, 0:4, :] = mean
        out[i, 4:8, :] = square


def stack_body(*refs):
    at = 0
    for ref in refs[:-1]:
        refs[-1][at : at + ref.shape[0], :] = ref[...]
        at += ref.shape[0]


def counts_body(bootstrap, counts):
    x, c = lax.axis_index("member_0"), lax.axis_index("member_1")
    shift = []
    for p in range(8):
        core = c if p < 4 else 1 - c
        member = lax.rem(x + 4 - ORDER[p % 4], 4) * 2 + core
        shift.append((member - p) * PIECE)
    picks = bootstrap[...]
    for k in range(ROWS // 128):
        first, last = 128 * k // PIECE, (128 * k + 127) // PIECE
        place = lax.broadcasted_iota(jnp.int32, (128, 1), 0) + 128 * k
        row_id = place + jnp.where(place < PIECE * (first + 1), shift[first], shift[last])
        hits = (picks == row_id).astype(F32)
        total = jnp.sum(hits, axis=1, keepdims=True)
        counts[:, 128 * k : 128 * k + 128] = jnp.broadcast_to(total, (128, 128)).T[0:8, :]


def lower_body(w1, b1, w1t, spare):
    spare[...] = jnp.zeros(spare.shape, F32)
    spare[0 : IN - 384, :] = w1[0, 384:IN, :].astype(F32)
    left = b1[...]
    for i in range(3):
        part = left.astype(BF16).astype(F32)
        spare[IN - 384 + i : IN - 383 + i, :] = part
        left = left - part
    for t in range(3):
        w1t[:, 128 * t : 128 * t + 128] = (w1[0, 128 * t : 128 * t + 128, :].astype(F32) * 0.5).astype(BF16).T
    w1t[:, 384:512] = (spare[...] * 0.5).astype(BF16).T


def as_column(row, n):
    return jnp.concatenate(
        [jnp.broadcast_to(row[:, 128 * t : 128 * t + 128], (128, 128)).T for t in range(n // 128)], axis=0
    )


def twice(x):
    return jnp.concatenate([x, x], axis=1)


def folded(x):
    return x[:, 0:128] + x[:, 128:256]


def step_body(
    near, far, other_near_hbm, other_far_hbm, stats, counts, w1t, w2_in, b2, lv, send, xs, hidden, slope, weighted, pre, odd, other_near, other_far, w2, w2t, row, arrived
):
    arrivals = [
        pltpu.make_async_copy(other_near_hbm, other_near, arrived.at[0]),
        pltpu.make_async_copy(other_far_hbm, other_far, arrived.at[1]),
    ]
    for arrival in arrivals:
        arrival.start()
    w2[:, 256:384] = jnp.zeros((H, 128), BF16)
    w2[:, 0:OUT] = w2_in[0]
    w2t[...] = w2[...].T
    row[...] = jnp.zeros(row.shape, F32)
    row[0:1, 0:OUT] = b2[...]
    row[1:2, 0:OUT] = lv[...]
    bias_o = as_column(row[0:1, :], OUT_PAD)
    mean, square = merged(stats[...], float(PIECE * 16))
    scale = 1.0 / jnp.sqrt(square * (1.0 / TOTAL) + 1e-06)

    def rescale(first, src):
        for t in range(4):
            lanes = slice(128 * t, 128 * t + 128)
            v = (src[:, lanes].astype(F32) - mean[t : t + 1, :]) * scale[t : t + 1, :]
            if t == 3:
                lane = lax.broadcasted_iota(jnp.int32, v.shape, 1)
                v = jnp.where((lane >= IN - 384) & (lane < IN - 381), 1.0, v)
            xs[first : first + src.shape[0], lanes] = v.astype(BF16)

    rescale(0, near)
    rescale(NEAR, far)
    log_var = as_column(row[1:2, :], OUT_PAD)
    shrink = twice(jnp.exp(-log_var))
    err_sum = jnp.zeros((OUT_PAD, 128), F32)
    off_sum = jnp.zeros((OUT_PAD, 128), F32)
    for i in range(ROWS // CHUNK):
        sources = (near, far) if i < 3 else (other_near, other_far)
        if i == 3:
            for arrival in arrivals:
                arrival.wait()
            rescale(768, other_near)
            rescale(768 + NEAR, other_far)
        start = CHUNK * (i % 3)
        if start + CHUNK <= NEAR:
            goal = sources[0][start : start + CHUNK, 512:896]
        else:
            goal = jnp.concatenate([sources[0][start:NEAR, 512:896], sources[1][:, 512:896]], axis=0)
        here = slice(CHUNK * i, CHUNK * i + CHUNK)
        count = counts[0:1, here]
        for h in range(0, H, BLOCK):
            block = slice(h, h + BLOCK)
            halved = lax.dot_general(
                w1t[block, :], xs[here, :], (((1,), (1,)), ((), ())), preferred_element_type=F32
            )
            twofold = jnp.tanh(halved) + 1.0
            value = halved * twofold
            gate = 0.5 * twofold
            hidden[block, here] = value.astype(BF16)
            slope[block, :] = (gate + value) - value * gate
        goal = goal.astype(F32).T
        pred = jnp.dot(w2t[...], hidden[:, here], preferred_element_type=F32) + twice(bias_o)
        residual = pred - goal
        scaled = residual * shrink
        err_sum += folded(residual * scaled * count)
        grad = scaled * (1.0 / ROWS)
        weighed = grad * count
        off_sum += folded(weighed)
        weighted[:, here] = weighed.astype(BF16)
        for h in range(0, H, BLOCK):
            block = slice(h, h + BLOCK)
            back = jnp.dot(w2[block, :], weighted[:, here], preferred_element_type=F32)
            pre[block, here] = (back * slope[block, :]).astype(BF16)
    upper = lax.dot_general(hidden[...], weighted[...], (((1,), (1,)), ((), ())), preferred_element_type=F32)
    lower = jnp.dot(pre[...], xs[...], preferred_element_type=F32)
    lane = lax.broadcasted_iota(jnp.int32, (H, 128), 1)
    tail = lower[:, 384:512]
    filled = jnp.where(lane >= OUT - 256, pltpu.roll(tail, OUT - 256, axis=1), upper[:, 256:384])
    bias = pltpu.roll(tail, 6, axis=1)
    rest = jnp.where((lane >= 12) & (lane < 15), pltpu.roll(tail, 5, axis=1), 0.0)
    rest = jnp.where(lane == 15, bias - bias.astype(BF16).astype(F32), rest)
    blocks = [upper[:, 0:128], upper[:, 128:256], filled] + [lower[:, 128 * j : 128 * j + 128] for j in range(3)]
    blocks = [block.astype(BF16) for block in blocks]
    second = lax.axis_index("member_1") == 1
    for z in range(8):
        for y in range(8):
            a, b = jnp.where(second, y, z), jnp.where(second, z, y)
            at = (z * 8 + y) * 16
            for j in range(6):
                send[a, pl.ds(pl.multiple_of(b * TILE + 16 * j, 16), 16), :] = blocks[j][at : at + 16, :]
            odd[pl.ds(pl.multiple_of(a * 128 + b * 16, 16), 16), :] = rest[at : at + 16, :]
    err_col = jnp.sum(err_sum, axis=1, keepdims=True)
    off_col = jnp.sum(off_sum, axis=1, keepdims=True)
    feature = lax.broadcasted_iota(jnp.int32, (OUT_PAD, 1), 0)
    real = feature < OUT
    loss = 0.5 * jnp.sum(jnp.where(real, err_col + ROWS * log_var[:, 0:1], 0.0), axis=0, keepdims=True) * (1.0 / ROWS)
    noise_col = jnp.where(feature == OUT, loss, 0.5 * (ROWS - err_col) * (1.0 / ROWS))
    vectors = jnp.zeros((128, 128), F32)
    lane = lax.broadcasted_iota(jnp.int32, (128, 128), 1)
    for t in range(3):
        for i, col in enumerate((off_col, noise_col)):
            part = col[128 * t : 128 * t + 128, :]
            high = part.astype(BF16).astype(F32)
            vectors = jnp.where(lane == 4 * t + 2 * i, high, vectors)
            vectors = jnp.where(lane == 4 * t + 2 * i + 1, part - high, vectors)
    vectors = vectors.T[0:16, :]
    for a in range(8):
        send[a, 8 * TILE : 8 * TILE + 16, :] = (vectors + odd[128 * a : 128 * a + 128, :].T[0:16, :]).astype(BF16)


def middle_body(got, send):
    for b in range(8):
        at = slice(b * TILE, b * TILE + TILE)
        send[b, 0:TILE, :] = jnp.sum(got[:, at, :].astype(F32), axis=0)
    last = jnp.sum(got[:, 8 * TILE : 8 * TILE + 16, :].astype(F32), axis=0)
    rows = [last[2 * i : 2 * i + 1, :] + last[2 * i + 1 : 2 * i + 2, :] for i in range(6)]
    bias = last[14:15, :] + last[15:16, :]
    turned = jnp.concatenate([last, jnp.zeros((112, 128), F32)], axis=0).T
    for b in range(8):
        send[b, TILE : TILE + 16, :] = turned[16 * b : 16 * b + 16, :]
        for i in range(6):
            send[b, TILE + 16 + i : TILE + 17 + i, :] = rows[i]
        send[b, TILE + 22 : TILE + 23, :] = pltpu.roll(bias, (128 - 16 * b) % 128, axis=1)
        send[b, TILE + 23 : TILE + 24, :] = jnp.zeros((1, 128), F32)


def finish_body(got, lower, bias, upper, offset, noise, loss):
    total = jnp.sum(got[...], axis=0)
    at = TILE + 16
    for j in range(3):
        width = min(128, OUT - 128 * j)
        upper[0, :, 128 * j : 128 * j + width] = total[16 * j : 16 * j + 16, 0:width]
        lower[0, :, 128 * j : 128 * j + 128] = total[48 + 16 * j : 64 + 16 * j, :]
        offset[:, 128 * j : 128 * j + width] = total[at + 2 * j : at + 2 * j + 1, 0:width]
        noise[:, 128 * j : 128 * j + width] = total[at + 2 * j + 1 : at + 2 * j + 2, 0:width]
    lower[0, :, 384:391] = total[32:48, OUT - 256 : 128]
    lower[0, :, 391:393] = total[TILE : TILE + 16, 12:14]
    bias[...] = total[at + 6 : at + 7, 0:16]
    loss[...] = total[at + 5 : at + 6, OUT - 256 : OUT - 255]


def exchange(x, **kw):
    return lax.all_to_all(x, kw.pop("axes"), 0, 0, tiled=True, **kw)


def per_device(inputs, targets, bootstrap, lower_weight, lower_shift, upper_weight, upper_shift, log_var):
    both, stats = call(
        prepare_body,
        (shape(PIECE, 896, dtype=BF16), shape(16, 8, 128)),
        2,
        scratch=(pltpu.VMEM((PIECE, IN), BF16), pltpu.VMEM((PIECE, OUT), BF16), pltpu.SemaphoreType.DMA((2,))),
        far=(0, 1),
        limit=54,
    )(inputs, targets)
    right, left = [(i, (i + 1) % 4) for i in range(4)], [(i, (i + 3) % 4) for i in range(4)]
    below = lax.ppermute(both, "member_0", right)
    above = lax.ppermute(both, "member_0", left)
    far_top = lax.ppermute(below[: PIECE // 2], "member_0", right)
    far_bottom = lax.ppermute(above[PIECE // 2 :], "member_0", left)
    stats = exchange(stats, axes=("dp_1", "member_1"))
    stats = call(merge_body, shape(32, 8, 128), 1)(stats)
    stats = exchange(stats, axes=("dp_0", "member_0"))
    near = call(stack_body, shape(NEAR, 896, dtype=BF16), 3)(both, below, above)
    other_near = lax.ppermute(near, "member_1", [(0, 1), (1, 0)])
    far = call(stack_body, shape(PIECE, 896, dtype=BF16), 2)(far_top, far_bottom)
    other_far = lax.ppermute(far, "member_1", [(0, 1), (1, 0)])
    counts = call(counts_body, shape(8, ROWS), 1, flops=5_000_000)(bootstrap)
    w1t = call(lower_body, shape(H, IN_PAD, dtype=BF16), 2, scratch=(pltpu.VMEM((128, H), F32),))(
        lower_weight, lower_shift
    )
    send = call(
        step_body,
        shape(8, 8 * TILE + 16, 128, dtype=BF16),
        10,
        scratch=(
            pltpu.VMEM((ROWS, IN_PAD), BF16),
            pltpu.VMEM((H, ROWS), BF16),
            pltpu.VMEM((H, CHUNK), F32),
            pltpu.VMEM((OUT_PAD, ROWS), BF16),
            pltpu.VMEM((H, ROWS), BF16),
            pltpu.VMEM((H, 128), F32),
            pltpu.VMEM((NEAR, 896), BF16),
            pltpu.VMEM((PIECE, 896), BF16),
            pltpu.VMEM((H, OUT_PAD), BF16),
            pltpu.VMEM((OUT_PAD, H), BF16),
            pltpu.VMEM((8, OUT_PAD), F32),
            pltpu.SemaphoreType.DMA((2,)),
        ),
        far=(2, 3),
        flops=7_000_000_000,
        moved=10_000_000,
        limit=24,
    )(near, far, other_near, other_far, stats, counts, w1t, upper_weight, upper_shift, log_var)
    got = exchange(send, axes=ALL, axis_index_groups=FIRST)
    send = call(middle_body, shape(8, TILE + 24, 128), 1)(got)
    got = exchange(send, axes=ALL, axis_index_groups=SECOND)
    lower_grad, bias_grad, upper_grad, offset_grad, noise_grad, member_loss = call(
        finish_body,
        (shape(1, 16, IN), shape(1, 16), shape(1, 16, OUT), shape(1, OUT), shape(1, OUT), shape(1, 1)),
        1,
    )(got)
    return (lower_grad, bias_grad, upper_grad, offset_grad, noise_grad, member_loss.reshape(1))


def solution(mesh):
    finer = Mesh(mesh.devices.reshape(8, 8, 4, 2), ALL)
    return jax.shard_map(
        per_device,
        mesh=finer,
        in_specs=(
            P(ALL, None),
            P(ALL, None),
            P(MEMBER, DP),
            P(MEMBER, None, None),
            P(MEMBER, None),
            P(MEMBER, None, None),
            P(MEMBER, None),
            P(MEMBER, None),
        ),
        out_specs=(
            P(MEMBER, DP, None),
            P(MEMBER, DP),
            P(MEMBER, DP, None),
            P(MEMBER, None),
            P(MEMBER, None),
            P(MEMBER),
        ),
        check_vma=False,
    )
```
